32 devices in a mesh: rep: 8 (over y, x, core), shard: 4 (over z).
Axes of the slice: x: 2, y: 2, z: 4, core: 2. Of those that a mesh axis runs over, the one named last changes fastest.
Arguments:
- tokens: bfloat16 [32, 128, 1536], P(('rep', 'shard')), may hold values from -6 to 6
- cotangent: bfloat16 [32, 128, 1536], P(('rep', 'shard')), may hold values from -6 to 6
- lengths: int32 [32], replicated, may hold values from 1 to 128, 3072 in all
- deal_order: int32 [32], replicated, may hold values from 0 to 31, as said below
- attention_gain: bfloat16 [2, 1536], P(None, 'shard'), may hold values from 0.099609375 to 1.8984375
- query_weight: bfloat16 [2, 1536, 1536], P(None, 'shard'), may hold values from -0.15625 to 0.15625
- key_weight: bfloat16 [2, 1536, 768], P(None, 'shard'), may hold values from -0.15625 to 0.15625
- value_weight: bfloat16 [2, 1536, 768], P(None, 'shard'), may hold values from -0.15625 to 0.15625
- output_weight: bfloat16 [2, 1536, 1536], P(None, 'shard'), may hold values from -0.625 to 0.625
- feedforward_gain: bfloat16 [2, 1536], P(None, 'shard'), may hold values from 0.099609375 to 1.8984375
- gate_weight: bfloat16 [2, 1536, 4096], P(None, 'shard'), may hold values from -0.15625 to 0.15625
- up_weight: bfloat16 [2, 1536, 4096], P(None, 'shard'), may hold values from -0.15625 to 0.15625
- down_weight: bfloat16 [2, 4096, 1536], P(None, 'shard'), may hold values from -0.09375 to 0.09375
Outputs:
- layer_output: bfloat16 [32, 128, 1536], P(('rep', 'shard'))
- input_grad: bfloat16 [32, 128, 1536], P(('rep', 'shard'))
- attention_gain_grad: float32 [2, 1536], P(None, 'shard')
- query_weight_grad: float32 [2, 1536, 1536], P(None, 'shard')
- key_weight_grad: float32 [2, 1536, 768], P(None, 'shard')
- value_weight_grad: float32 [2, 1536, 768], P(None, 'shard')
- output_weight_grad: float32 [2, 1536, 1536], P(None, 'shard')
- feedforward_gain_grad: float32 [2, 1536], P(None, 'shard')
- gate_weight_grad: float32 [2, 1536, 4096], P(None, 'shard')
- up_weight_grad: float32 [2, 1536, 4096], P(None, 'shard')
- down_weight_grad: float32 [2, 4096, 1536], P(None, 'shard')
The draws below stay inside these ranges and needn't reach their ends.
Inputs may be any that keep to these rules, and one draw needn't show every extreme that they name: deal_order is a permutation of the sequences with deal_order[j] % 4 == j % 4. `lengths`: the longest sequence fills all 128 slots.
All inputs are finite; a program needn't handle non-finite values.
Results may differ from the reference program's by a relative error of at most 0.028.
Values may be sent and summed in bfloat16 or wider, within the bound.
A program may use at most 448 MiB of HBM per device.

```python
import math
import jax
import jax.numpy as jnp
import numpy as np
from jax import lax

D = 1536
HEADS = 16
KV_HEADS = 8
HEAD = 96
FF = 4096
LEN = 128
LAYERS = 2
SEQS = 32
N_SHARD = 4


def draw_deal_order(key, part):
    replica_count = SEQS // N_SHARD
    column_keys = jax.random.split(jax.random.fold_in(key, 17), N_SHARD)

    def column_order(column_key):
        return jax.random.permutation(column_key, replica_count)
    orders = jax.vmap(column_order)(column_keys)
    dealt = orders.T * N_SHARD + jnp.arange(N_SHARD)[None, :]
    return dealt.reshape(-1).astype(jnp.int32)


def shard_levels(rng, dims, cuts, smallest, largest):
    level, own = 1.0, jax.random.fold_in(rng, 6)
    for dim, blocks in cuts:
        heights = jnp.exp(jax.random.uniform(jax.random.fold_in(own, dim), (blocks,), jnp.float32, smallest / len(cuts), largest / len(cuts)))
        level = level * jnp.repeat(heights, dims[dim] // blocks).reshape([-1 if axis == dim else 1 for axis in range(len(dims))])
    return level


def profile(count, total, most, lean):
    portions = [(1 << 20) // math.isqrt(rank ** lean) + 1 for rank in range(2, count + 1)]
    spare, holding = total - most - (count - 1), [1] * (count - 1)
    while spare > 0:
        movable = [i for i in range(count - 1) if holding[i] < most]
        whole, remaining = sum([portions[i] for i in movable]), spare
        for i in movable:
            addition = min(most - holding[i], max(1, remaining * portions[i] // whole), spare)
            holding[i] = holding[i] + addition
            spare = spare - addition
    return np.array([most] + holding)


def ragged_sizes(rng, count, total, bound, slope):
    if count == 2:
        one = jax.random.randint(rng, (), max(1, total - bound), min(bound, total - 1) + 1)
        return jnp.stack([one, total - one])
    sizes = jnp.asarray(profile(count, total, bound, slope), jnp.int32)
    pairs = (count - 1) // 2
    donor, receiver = sizes[1:1 + 2 * pairs:2], sizes[2:2 + 2 * pairs:2]
    room = jnp.minimum(donor - 1, bound - receiver)
    moved = jax.random.randint(jax.random.fold_in(rng, 1), (pairs,), 0, 1 << 20) % (room + 1)
    sizes = sizes.at[1:1 + 2 * pairs:2].set(donor - moved).at[2:2 + 2 * pairs:2].set(receiver + moved)
    return sizes[jax.random.permutation(jax.random.fold_in(rng, 2), count)]


def scatter_about(key, shape, width, limit, cuts=(), held_as=jnp.bfloat16):
    values = width * jax.random.normal(key, shape, jnp.float32)
    if cuts:
        values = values * shard_levels(key, shape, cuts, -0.22, 0.18)
    return jnp.clip(values, -limit, limit).astype(held_as)


def setup_inputs(seed: int = 0) -> dict:
    splits = jax.random.split(jax.random.key(seed), 14)
    tokens = scatter_about(splits[0], (SEQS, LEN, D), 1.0, 6.0, ((0, 32),))
    cotangent = scatter_about(splits[1], (SEQS, LEN, D), 1.0, 6.0, ((0, 32),))
    lengths = ragged_sizes(splits[2], SEQS, SEQS * LEN * 3 // 4, LEN, 1).astype(jnp.int32)
    deal_order = draw_deal_order(jax.random.fold_in(splits[13], 71), 0)
    attention_gain = jnp.clip(1.0 + 0.18 * jax.random.normal(splits[4], (LAYERS, D), jnp.float32), 0.099609375, 1.8984375).astype(jnp.bfloat16)
    query_weight = scatter_about(splits[5], (LAYERS, D, HEADS * HEAD), D ** -0.5, 0.15625, ((1, 4),))
    key_weight = scatter_about(splits[6], (LAYERS, D, KV_HEADS * HEAD), D ** -0.5, 0.15625, ((1, 4),))
    value_weight = scatter_about(splits[7], (LAYERS, D, KV_HEADS * HEAD), D ** -0.5, 0.15625, ((1, 4),))
    output_weight = scatter_about(splits[8], (LAYERS, HEADS * HEAD, D), (HEADS * HEAD // 16) ** -0.5, 0.625, ((1, 4),))
    feedforward_gain = jnp.clip(1.0 + 0.18 * jax.random.normal(splits[9], (LAYERS, D), jnp.float32), 0.099609375, 1.8984375).astype(jnp.bfloat16)
    gate_weight = scatter_about(splits[10], (LAYERS, D, FF), D ** -0.5, 0.15625, ((1, 4),))
    up_weight = scatter_about(splits[11], (LAYERS, D, FF), D ** -0.5, 0.15625, ((1, 4),))
    down_weight = scatter_about(splits[12], (LAYERS, FF, D), FF ** -0.5, 0.09375, ((1, 4),))
    return dict(tokens=tokens, cotangent=cotangent, lengths=lengths, deal_order=deal_order, attention_gain=attention_gain, query_weight=query_weight, key_weight=key_weight, value_weight=value_weight, output_weight=output_weight, feedforward_gain=feedforward_gain, gate_weight=gate_weight, up_weight=up_weight, down_weight=down_weight)


epsilon = 1e-05
rope_base = 100000.0
masked_score = -1e+30

@jax.custom_vjp
def low(v):
    return lax.optimization_barrier(v.astype(jnp.bfloat16)).astype(jnp.float32)

@jax.custom_vjp
def low_back(v):
    return v

def low_keep(v):
    return (low(v), None)

def low_pass(kept, grad):
    return (grad,)

def back_keep(v):
    return (v, None)

def back_low(kept, grad):
    return (low(grad),)
low.defvjp(low_keep, low_pass)
low_back.defvjp(back_keep, back_low)

def matmul(left, right):
    return jnp.dot(left, right, precision=lax.Precision.HIGHEST, preferred_element_type=jnp.float32)

def rope_tables(row_count):
    position = jnp.arange(row_count).astype(jnp.float32)
    frequency = rope_base ** (-(2.0 * jnp.arange(HEAD // 2).astype(jnp.float32)) / HEAD)
    angles = position[:, None] * frequency[None, :]
    angles = jnp.concatenate([angles, angles], axis=1)
    return (jnp.cos(angles)[:, None, :], jnp.sin(angles)[:, None, :])

def rotate(vector, cosine, sine):
    halfway = vector.shape[-1] // 2
    turned = jnp.concatenate([-vector[..., halfway:], vector[..., :halfway]], axis=-1)
    return vector * cosine + turned * sine

def rms_scale(stream):
    return lax.rsqrt(lax.optimization_barrier(jnp.mean(stream * stream, axis=-1, keepdims=True)) + epsilon)

def block_forward(stream, params, mask, cosine, sine):
    attention_gain, query_weight, key_weight, value_weight, output_weight, feedforward_gain, gate_weight, up_weight, down_weight = params
    row_count = stream.shape[0]
    group_size = HEADS // KV_HEADS
    normed = low(stream * rms_scale(stream) * attention_gain)
    queries = low_back(matmul(normed, query_weight)).reshape(row_count, HEADS, HEAD)
    queries = low(rotate(queries, cosine, sine)).reshape(row_count, KV_HEADS, group_size, HEAD)
    keys_rot = low_back(matmul(normed, key_weight)).reshape(row_count, KV_HEADS, HEAD)
    keys_rot = low(rotate(keys_rot, cosine, sine))
    values = low(low_back(matmul(normed, value_weight))).reshape(row_count, KV_HEADS, HEAD)
    scores = jnp.einsum('qkgd,tkd->kgqt', queries, keys_rot, precision=lax.Precision.HIGHEST) * HEAD ** (-0.5)
    scores = jnp.where(mask, low_back(scores), masked_score)
    row_max = lax.optimization_barrier(jnp.max(scores, axis=-1, keepdims=True))
    shifted = jnp.exp(scores - row_max)
    attention = shifted / lax.optimization_barrier(jnp.sum(shifted, axis=-1, keepdims=True))
    mixed = jnp.einsum('kgqt,tkd->qkgd', low(attention), values, precision=lax.Precision.HIGHEST)
    mixed = low(low_back(mixed.reshape(row_count, HEADS * HEAD)))
    middle = stream + low_back(matmul(mixed, output_weight))
    normed_two = low(middle * rms_scale(middle) * feedforward_gain)
    gate_lin = low_back(matmul(normed_two, gate_weight))
    up_lin = low_back(matmul(normed_two, up_weight))
    hidden = low(gate_lin * jax.nn.sigmoid(gate_lin) * up_lin)
    return middle + low_back(matmul(hidden, down_weight))

def reference(tokens, cotangent, lengths, deal_order, attention_gain, query_weight, key_weight, value_weight, output_weight, feedforward_gain, gate_weight, up_weight, down_weight):
    params = tuple((weight.astype(jnp.float32) for weight in (attention_gain, query_weight, key_weight, value_weight, output_weight, feedforward_gain, gate_weight, up_weight, down_weight)))
    cosine, sine = rope_tables(LEN)
    position = jnp.arange(LEN).astype(jnp.int32)

    def one_sequence(totals, slot):
        source = deal_order[slot].astype(jnp.int32)
        length = lengths[source]
        valid = (position < length)[:, None]
        mask = (position[None, :] <= position[:, None]) & (position[None, :] < length)

        def forward(weights, stream):
            for layer_index in range(LAYERS):
                stream = block_forward(stream, tuple((single[layer_index] for single in weights)), mask, cosine, sine)
            return jnp.where(valid, stream, 0.0)
        outcome, pullback = jax.vjp(forward, params, tokens[source].astype(jnp.float32))
        weight_grads, input_part = pullback(cotangent[slot].astype(jnp.float32))
        totals = jax.tree.map(lambda running, latest: running + latest, totals, weight_grads)
        return (totals, (outcome.astype(jnp.bfloat16), input_part.astype(jnp.bfloat16)))
    zeros = tuple((jnp.zeros_like(single) for single in params))
    totals, (outputs, input_parts) = lax.scan(one_sequence, zeros, jnp.arange(SEQS).astype(jnp.int32))
    input_grad = jnp.zeros_like(input_parts).at[deal_order.astype(jnp.int32)].set(input_parts)
    return (outputs, input_grad, totals[0], totals[1], totals[2], totals[3], totals[4], totals[5], totals[6], totals[7], totals[8])
```

```python
import functools
import jax
import jax.numpy as jnp
from jax import lax
from jax.experimental import pallas as pl
from jax.experimental.pallas import tpu as pltpu
from jax.sharding import PartitionSpec as P

HEADS = 16
KV_HEADS = 8
HEAD = 96
LAYERS = 2


epsilon = 1e-05
rope_base = 100000.0
masked_score = -1e30


def rope_tables(row_count):
    position = jnp.arange(row_count).astype(jnp.float32)
    frequency = rope_base ** (-(2.0 * jnp.arange(HEAD // 2).astype(jnp.float32)) / HEAD)
    angles = position[:, None] * frequency[None, :]
    angles = jnp.concatenate([angles, angles], axis=1)
    return (jnp.cos(angles)[:, None, :], jnp.sin(angles)[:, None, :])


def rotate(vector, cosine, sine):
    halfway = vector.shape[-1] // 2
    turned = jnp.concatenate([-vector[..., halfway:], vector[..., :halfway]], axis=-1)
    return vector * cosine + turned * sine


def unrotate(vector, cosine, sine):
    halfway = vector.shape[-1] // 2
    scaled = vector * sine
    turned = jnp.concatenate([scaled[..., halfway:], -scaled[..., :halfway]], axis=-1)
    return vector * cosine + turned


def rms_scale(stream):
    return lax.rsqrt(jnp.mean(stream * stream, axis=-1, keepdims=True) + epsilon)


def left_product(left, right):
    return jnp.dot(left, right, preferred_element_type=jnp.float32)


def right_transposed(grad_rows, weight):
    return jnp.einsum("lf,df->ld", grad_rows, weight, preferred_element_type=jnp.float32)


def row_sum_product(inputs, grad_rows):
    return jnp.einsum("ld,lf->df", inputs, grad_rows, preferred_element_type=jnp.float32)


def norm_backward(normed_grad, stream, scale, gain):
    gain_grad = jnp.sum(normed_grad * stream * scale, axis=0)
    weighted = normed_grad * gain.astype(jnp.float32)
    stream_grad = scale * weighted - stream * (scale * scale * scale) * jnp.mean(
        weighted * stream, axis=-1, keepdims=True
    )
    return (gain_grad, stream_grad)


def pick_sequence(wanted, carry, piece):
    span_rows = piece.shape[0]
    inside = (wanted >= 0) & (wanted < span_rows)
    chosen = lax.dynamic_slice_in_dim(piece, jnp.clip(wanted, 0, span_rows - 1), 1, 0)
    return jnp.where(inside, chosen, carry)


def gather_forward(stacked, layer_index):
    return (
        lax.all_gather(stacked[0][layer_index], "shard", axis=0, tiled=True),
        lax.all_gather(stacked[1][layer_index], "shard", axis=0, tiled=True),
        lax.all_gather(stacked[2][layer_index], "shard", axis=0, tiled=True),
        lax.all_gather(stacked[3][layer_index], "shard", axis=0, tiled=True),
        lax.all_gather(stacked[4][layer_index], "shard", axis=0, tiled=True),
        lax.all_gather(stacked[5][layer_index], "shard", axis=0, tiled=True),
        lax.all_gather(stacked[6][layer_index], "shard", axis=0, tiled=True),
        lax.all_gather(stacked[7][layer_index], "shard", axis=0, tiled=True),
        lax.all_gather(stacked[8][layer_index], "shard", axis=0, tiled=True),
    )


def gather_backward(stacked, layer_index):
    return (
        lax.all_gather(stacked[0][layer_index], "shard", axis=0, tiled=True),
        lax.all_gather(stacked[1][layer_index], "shard", axis=0, tiled=True),
        lax.all_gather(stacked[2][layer_index], "shard", axis=0, tiled=True),
        lax.all_gather(stacked[3][layer_index], "shard", axis=0, tiled=True),
        lax.all_gather(stacked[4][layer_index], "shard", axis=0, tiled=True),
        lax.all_gather(stacked[5][layer_index], "shard", axis=0, tiled=True),
        lax.all_gather(stacked[6][layer_index], "shard", axis=0, tiled=True),
        lax.all_gather(stacked[7][layer_index], "shard", axis=0, tiled=True),
        lax.all_gather(stacked[8][layer_index], "shard", axis=0, tiled=True),
    )


def attention_scores(queries, keys_rot, mask):
    scores = jnp.einsum(
        "qkgd,tkd->kgqt", queries, keys_rot, preferred_element_type=jnp.float32
    ) * HEAD ** (-0.5)
    return jnp.where(mask, scores, masked_score)


def layer_forward(stream, weights, mask, cosine, sine):
    (
        attention_gain,
        query_weight,
        key_weight,
        value_weight,
        output_weight,
        feedforward_gain,
        gate_weight,
        up_weight,
        down_weight,
    ) = weights
    row_count = stream.shape[0]
    group_size = HEADS // KV_HEADS
    scale_one = rms_scale(stream)
    normed_one = (stream * scale_one * attention_gain.astype(jnp.float32)).astype(jnp.bfloat16)
    queries = left_product(normed_one, query_weight).reshape(row_count, HEADS, HEAD)
    queries = (
        rotate(queries, cosine, sine)
        .astype(jnp.bfloat16)
        .reshape(row_count, KV_HEADS, group_size, HEAD)
    )
    keys_rot = left_product(normed_one, key_weight).reshape(row_count, KV_HEADS, HEAD)
    keys_rot = rotate(keys_rot, cosine, sine).astype(jnp.bfloat16)
    values = (
        left_product(normed_one, value_weight)
        .astype(jnp.bfloat16)
        .reshape(row_count, KV_HEADS, HEAD)
    )
    scores = attention_scores(queries, keys_rot, mask)
    row_max = jnp.max(scores, axis=-1, keepdims=True)
    shifted = jnp.exp(scores - row_max)
    row_total = jnp.sum(shifted, axis=-1, keepdims=True)
    attention = shifted / row_total
    log_total = row_max + jnp.log(row_total)
    mixed = jnp.einsum(
        "kgqt,tkd->qkgd", attention.astype(jnp.bfloat16), values, preferred_element_type=jnp.float32
    )
    mixed = mixed.reshape(row_count, HEADS * HEAD).astype(jnp.bfloat16)
    middle = stream + left_product(mixed, output_weight)
    scale_two = rms_scale(middle)
    normed_two = (middle * scale_two * feedforward_gain.astype(jnp.float32)).astype(jnp.bfloat16)
    gate_lin = left_product(normed_two, gate_weight)
    up_lin = left_product(normed_two, up_weight)
    hidden = (gate_lin * jax.nn.sigmoid(gate_lin) * up_lin).astype(jnp.bfloat16)
    result_stream = middle + left_product(hidden, down_weight)
    kept = (
        stream,
        scale_one,
        normed_one,
        queries,
        keys_rot,
        values,
        log_total,
        mixed,
        middle,
        scale_two,
        normed_two,
        gate_lin,
        up_lin,
        hidden,
    )
    return (result_stream, kept)


def layer_backward(grad_out, weights, kept, mask, cosine, sine):
    (
        attention_gain,
        query_weight,
        key_weight,
        value_weight,
        output_weight,
        feedforward_gain,
        gate_weight,
        up_weight,
        down_weight,
    ) = weights
    (
        stream,
        scale_one,
        normed_one,
        queries,
        keys_rot,
        values,
        log_total,
        mixed,
        middle,
        scale_two,
        normed_two,
        gate_lin,
        up_lin,
        hidden,
    ) = kept
    row_count = stream.shape[0]
    group_size = HEADS // KV_HEADS
    branch_grad = grad_out.astype(jnp.bfloat16)
    hidden_grad = right_transposed(branch_grad, down_weight)
    down_grad = row_sum_product(hidden, branch_grad)
    sigma = jax.nn.sigmoid(gate_lin)
    gate_grad = (hidden_grad * up_lin * sigma * (1.0 + gate_lin * (1.0 - sigma))).astype(
        jnp.bfloat16
    )
    up_grad = (hidden_grad * gate_lin * sigma).astype(jnp.bfloat16)
    normed_grad = right_transposed(gate_grad, gate_weight) + right_transposed(up_grad, up_weight)
    gate_weight_grad = row_sum_product(normed_two, gate_grad)
    up_weight_grad = row_sum_product(normed_two, up_grad)
    forward_gain_grad, middle_part = norm_backward(normed_grad, middle, scale_two, feedforward_gain)
    middle_grad = grad_out + middle_part
    mlp_shares = (
        lax.psum_scatter(
            forward_gain_grad.astype(jnp.bfloat16), "shard", scatter_dimension=0, tiled=True
        ).astype(jnp.float32),
        lax.psum_scatter(
            gate_weight_grad.astype(jnp.bfloat16), "shard", scatter_dimension=0, tiled=True
        ).astype(jnp.float32),
        lax.psum_scatter(
            up_weight_grad.astype(jnp.bfloat16), "shard", scatter_dimension=0, tiled=True
        ).astype(jnp.float32),
        lax.psum_scatter(
            down_grad.astype(jnp.bfloat16), "shard", scatter_dimension=0, tiled=True
        ).astype(jnp.float32),
    )
    branch_grad = middle_grad.astype(jnp.bfloat16)
    mixed_grad = right_transposed(branch_grad, output_weight).astype(jnp.bfloat16)
    output_weight_grad = row_sum_product(mixed, branch_grad)
    mixed_grad = mixed_grad.reshape(row_count, KV_HEADS, group_size, HEAD)
    scores = attention_scores(queries, keys_rot, mask)
    attention = jnp.exp(scores - log_total)
    attention_grad = jnp.einsum(
        "qkgd,tkd->kgqt", mixed_grad, values, preferred_element_type=jnp.float32
    )
    value_grad = jnp.einsum(
        "kgqt,qkgd->tkd",
        attention.astype(jnp.bfloat16),
        mixed_grad,
        preferred_element_type=jnp.float32,
    )
    value_grad = value_grad.astype(jnp.bfloat16).reshape(row_count, KV_HEADS * HEAD)
    row_dot = jnp.sum(attention * attention_grad, axis=-1, keepdims=True)
    score_grad = (attention * (attention_grad - row_dot)).astype(jnp.bfloat16)
    query_grad = jnp.einsum(
        "kgqt,tkd->qkgd", score_grad, keys_rot, preferred_element_type=jnp.float32
    ) * HEAD ** (-0.5)
    key_grad = jnp.einsum(
        "kgqt,qkgd->tkd", score_grad, queries, preferred_element_type=jnp.float32
    ) * HEAD ** (-0.5)
    query_grad = (
        unrotate(query_grad.reshape(row_count, HEADS, HEAD), cosine, sine)
        .astype(jnp.bfloat16)
        .reshape(row_count, HEADS * HEAD)
    )
    key_grad = (
        unrotate(key_grad, cosine, sine).astype(jnp.bfloat16).reshape(row_count, KV_HEADS * HEAD)
    )
    normed_grad = (
        right_transposed(query_grad, query_weight)
        + right_transposed(key_grad, key_weight)
        + right_transposed(value_grad, value_weight)
    )
    query_weight_grad = row_sum_product(normed_one, query_grad)
    key_weight_grad = row_sum_product(normed_one, key_grad)
    value_weight_grad = row_sum_product(normed_one, value_grad)
    attend_gain_grad, stream_part = norm_backward(normed_grad, stream, scale_one, attention_gain)
    attention_shares = (
        lax.psum_scatter(
            attend_gain_grad.astype(jnp.bfloat16), "shard", scatter_dimension=0, tiled=True
        ).astype(jnp.float32),
        lax.psum_scatter(
            query_weight_grad.astype(jnp.bfloat16), "shard", scatter_dimension=0, tiled=True
        ).astype(jnp.float32),
        lax.psum_scatter(
            key_weight_grad.astype(jnp.bfloat16), "shard", scatter_dimension=0, tiled=True
        ).astype(jnp.float32),
        lax.psum_scatter(
            value_weight_grad.astype(jnp.bfloat16), "shard", scatter_dimension=0, tiled=True
        ).astype(jnp.float32),
        lax.psum_scatter(
            output_weight_grad.astype(jnp.bfloat16), "shard", scatter_dimension=0, tiled=True
        ).astype(jnp.float32),
    )
    return (middle_grad + stream_part, attention_shares + mlp_shares)


def whole_weight_shards(
    tokens,
    cotangent,
    lengths,
    deal_order,
    attention_gain,
    query_weight,
    key_weight,
    value_weight,
    output_weight,
    feedforward_gain,
    gate_weight,
    up_weight,
    down_weight,
):
    stacked = (
        attention_gain,
        query_weight,
        key_weight,
        value_weight,
        output_weight,
        feedforward_gain,
        gate_weight,
        up_weight,
        down_weight,
    )
    shard_count = lax.axis_size("shard")
    device = lax.axis_index(("rep", "shard"))
    wanted = deal_order[device]
    length = lengths[wanted]
    sequence = pick_sequence(
        wanted // shard_count,
        jnp.zeros_like(tokens),
        lax.all_gather(tokens, "rep", axis=0, tiled=True),
    )
    row_count = tokens.shape[1]
    position = jnp.arange(row_count)
    valid = (position < length)[:, None]
    mask = (position[None, :] <= position[:, None]) & (position[None, :] < length)
    cosine, sine = rope_tables(row_count)
    stream = sequence[0].astype(jnp.float32)
    kept_layers = []
    weights = None
    for layer_index in range(LAYERS):
        weights = gather_forward(stacked, layer_index)
        stream, kept = layer_forward(stream, weights, mask, cosine, sine)
        kept_layers.append(kept)
    layer_output = jnp.where(valid, stream, 0.0).astype(jnp.bfloat16)[None]
    grad_stream = jnp.where(valid, cotangent[0].astype(jnp.float32), 0.0)
    layer_shares = [None] * LAYERS
    for layer_index in reversed(range(LAYERS)):
        weights_back = gather_backward(stacked, layer_index)
        grad_stream, shares = layer_backward(
            grad_stream, weights_back, kept_layers[layer_index], mask, cosine, sine
        )
        layer_shares[layer_index] = shares
    grads = tuple(
        (jnp.stack([layer_shares[index][member] for index in range(LAYERS)]) for member in range(9))
    )
    grads = (
        lax.psum(grads[0].astype(jnp.bfloat16), "rep").astype(jnp.float32),
        lax.psum(grads[1].astype(jnp.bfloat16), "rep").astype(jnp.float32),
        lax.psum(grads[2].astype(jnp.bfloat16), "rep").astype(jnp.float32),
        lax.psum(grads[3].astype(jnp.bfloat16), "rep").astype(jnp.float32),
        lax.psum(grads[4].astype(jnp.bfloat16), "rep").astype(jnp.float32),
        lax.psum(grads[5].astype(jnp.bfloat16), "rep").astype(jnp.float32),
        lax.psum(grads[6].astype(jnp.bfloat16), "rep").astype(jnp.float32),
        lax.psum(grads[7].astype(jnp.bfloat16), "rep").astype(jnp.float32),
        lax.psum(grads[8].astype(jnp.bfloat16), "rep").astype(jnp.float32),
    )
    inverse = jnp.sum(jnp.where(deal_order == device, jnp.arange(deal_order.shape[0]), 0))
    input_grad = pick_sequence(
        inverse // shard_count,
        jnp.zeros_like(tokens),
        lax.all_gather(grad_stream.astype(jnp.bfloat16)[None], "rep", axis=0, tiled=True),
    )
    return (layer_output, input_grad) + tuple(grads)


PIECES = 4
MESH = pl.DeviceIdType.MESH


def plane_neighbours():
    place = lax.axis_index("rep")
    core, chip = place % 2, place // 2
    mate = place + 1 - 2 * core
    across = place + 2 - 4 * (chip % 2)
    along = place + 4 - 8 * (chip // 2)
    return (place, mate, across, along)


def remote(source, target, sems, kind, piece, place):
    send_sem, recv_sem = sems
    copy = pltpu.make_async_remote_copy(
        src_ref=source,
        dst_ref=target,
        send_sem=send_sem.at[kind, piece],
        recv_sem=recv_sem.at[kind, piece],
        device_id={"rep": place},
        device_id_type=MESH,
    )
    copy.start()
    return copy


def greet(places):
    barrier = pltpu.get_barrier_semaphore()
    for place in places:
        pl.semaphore_signal(barrier, inc=1, device_id=place, device_id_type=MESH)
    pl.semaphore_wait(barrier, len(places))


def piece_rows(piece, row_count):
    span = row_count // PIECES
    return (pl.ds(piece * span, span), pl.ds(piece * span, span // 2), pl.ds(piece * span + span // 2, span // 2))


def gather_send(full, sems, first_kind, piece, row_count):
    place, mate, across, along = plane_neighbours()
    rows, _, _ = piece_rows(piece, row_count)
    own = full.at[place, rows]
    return [
        remote(own, own, sems, first_kind, piece, mate),
        remote(own, own, sems, first_kind + 1, piece, across),
        remote(own, own, sems, first_kind + 2, piece, along),
    ]


def gather_finish(full, sems, first_kind, row_count, sent):
    place, mate, across, along = plane_neighbours()
    far = across + along - place
    passed = []
    for piece in range(PIECES):
        rows, upper, lower = piece_rows(piece, row_count)
        sent[piece][1].wait_recv()
        there = full.at[across, upper]
        whole = full.at[across, rows]
        to_along = remote(there, there, sems, first_kind + 3, piece, along)
        mate_one = remote(whole, whole, sems, first_kind + 5, piece, mate)
        sent[piece][2].wait_recv()
        there = full.at[along, lower]
        whole = full.at[along, rows]
        to_across = remote(there, there, sems, first_kind + 4, piece, across)
        mate_two = remote(whole, whole, sems, first_kind + 6, piece, mate)
        passed.append([to_along, to_across, mate_one, mate_two])
    for piece in range(PIECES):
        rows, _, _ = piece_rows(piece, row_count)
        passed[piece][0].wait_recv()
        passed[piece][1].wait_recv()
        whole = full.at[far, rows]
        passed[piece].append(remote(whole, whole, sems, first_kind + 7, piece, mate))
    for piece in range(PIECES):
        sent[piece][0].wait_recv()
        for copy in passed[piece][2:]:
            copy.wait_recv()
        for copy in sent[piece] + passed[piece]:
            copy.wait_send()


def scatter_stage(left, right, transposed, part, from_mate, send_far, send_across, send_along,
                  far_across, far_along, got_across, got_along, sems, finish):
    place, mate, across, along = plane_neighbours()
    core, chip = place % 2, place // 2
    far_chip, across_chip, along_chip = (across + along - place) // 2, across // 2, along // 2
    row_count, width = part.shape[2], part.shape[3]
    span = row_count // PIECES
    depth = left.shape[-1]
    wide = lambda ref, *index: ref[index].astype(jnp.float32)
    mates, fars, nears = [], [], []
    for piece in range(PIECES):
        rows, _, _ = piece_rows(piece, row_count)
        block = left[:, rows, :].reshape(-1, depth)
        product = lax.dot_general(
            block, right[...], (((1,), (1 if transposed else 0,)), ((), ())),
            preferred_element_type=jnp.float32,
        )
        part[:, :, rows, :] = product.astype(jnp.bfloat16).reshape(-1, 2, span, width)
        if piece == 0:
            greet([{"rep": mate}, {"rep": across}, {"rep": along}])
        mates.append(
            remote(part.at[:, 1 - core, rows, :], from_mate.at[:, rows, :], sems, 0, piece, mate)
        )
    for piece in range(PIECES):
        rows, upper, lower = piece_rows(piece, row_count)
        mates[piece].wait_recv()
        total = wide(part, far_chip, core, rows) + wide(from_mate, far_chip, rows)
        send_far[rows, :] = total.astype(jnp.bfloat16)
        fars.append([
            remote(send_far.at[upper], far_across.at[piece], sems, 1, piece, across),
            remote(send_far.at[lower], far_along.at[piece], sems, 2, piece, along),
        ])
    for piece in range(PIECES):
        rows, upper, lower = piece_rows(piece, row_count)
        fars[piece][0].wait_recv()
        total = wide(part, along_chip, core, upper) + wide(from_mate, along_chip, upper) + wide(far_across, piece)
        send_along[upper, :] = total.astype(jnp.bfloat16)
        total = wide(part, along_chip, core, lower) + wide(from_mate, along_chip, lower)
        send_along[lower, :] = total.astype(jnp.bfloat16)
        to_along = remote(send_along.at[rows], got_along.at[rows], sems, 4, piece, along)
        fars[piece][1].wait_recv()
        total = wide(part, across_chip, core, lower) + wide(from_mate, across_chip, lower) + wide(far_along, piece)
        send_across[lower, :] = total.astype(jnp.bfloat16)
        total = wide(part, across_chip, core, upper) + wide(from_mate, across_chip, upper)
        send_across[upper, :] = total.astype(jnp.bfloat16)
        to_across = remote(send_across.at[rows], got_across.at[rows], sems, 3, piece, across)
        nears.append([to_across, to_along])
    results = []
    for piece in range(PIECES):
        rows, _, _ = piece_rows(piece, row_count)
        nears[piece][0].wait_recv()
        nears[piece][1].wait_recv()
        total = (
            wide(part, chip, core, rows) + wide(from_mate, chip, rows)
            + wide(got_across, rows) + wide(got_along, rows)
        )
        results.append(finish(piece, rows, total))
    for piece in range(PIECES):
        for copy in [mates[piece]] + fars[piece] + nears[piece]:
            copy.wait_send()
    return results


def scatter_scratch(row_count, width):
    half = row_count // PIECES // 2
    return [
        pltpu.VMEM((4, 2, row_count, width), jnp.bfloat16),
        pltpu.VMEM((4, row_count, width), jnp.bfloat16),
        pltpu.VMEM((row_count, width), jnp.bfloat16),
        pltpu.VMEM((row_count, width), jnp.bfloat16),
        pltpu.VMEM((row_count, width), jnp.bfloat16),
        pltpu.VMEM((PIECES, half, width), jnp.bfloat16),
        pltpu.VMEM((PIECES, half, width), jnp.bfloat16),
        pltpu.VMEM((row_count, width), jnp.bfloat16),
        pltpu.VMEM((row_count, width), jnp.bfloat16),
        pltpu.SemaphoreType.DMA((13, PIECES)),
        pltpu.SemaphoreType.DMA((13, PIECES)),
    ]


def norm_scale(stream):
    return lax.rsqrt(jnp.mean(stream * stream, axis=-1, keepdims=True) + epsilon)


def forward_exchange(normed, left, right, stream, gain, full, middle, *scratch):
    sems = scratch[-2:]
    row_count = stream.shape[0]

    def finish(piece, rows, total):
        place = lax.axis_index("rep")
        stepped = stream[rows, :] + total
        middle[rows, :] = stepped
        if normed:
            stepped = stepped * norm_scale(stepped) * gain[...]
        full[place, rows, :] = stepped.astype(jnp.bfloat16)
        return gather_send(full, sems, 5, piece, row_count)

    sent = scatter_stage(left, right, False, *scratch[:-2], sems, finish)
    gather_finish(full, sems, 5, row_count, sent)


def backward_exchange(spread, left, right, grad, stream, gain, *rest):
    if spread:
        full, stepped_ref, gain_grad = rest[:3]
        scratch = rest[3:]
    else:
        stepped_ref, gain_grad = rest[:2]
        scratch = rest[2:]
    sems = scratch[-2:]
    row_count = stream.shape[0]

    def finish(piece, rows, total):
        place = lax.axis_index("rep")
        held = stream[rows, :]
        scale = norm_scale(held)
        weighted = total * gain[...]
        stepped = (
            grad[rows, :] + scale * weighted
            - held * (scale * scale * scale) * jnp.mean(weighted * held, axis=-1, keepdims=True)
        )
        share = jnp.sum(total * held * scale, axis=0, keepdims=True)
        gain_grad[...] = share if piece == 0 else gain_grad[...] + share
        stepped_ref[rows, :] = stepped.astype(stepped_ref.dtype)
        if not spread:
            return None
        full[place, rows, :] = stepped.astype(jnp.bfloat16)
        return gather_send(full, sems, 5, piece, row_count)

    sent = scatter_stage(left, right, True, *scratch[:-2], sems, finish)
    if spread:
        gather_finish(full, sems, 5, row_count, sent)


def vmem_specs(count):
    return [pl.BlockSpec(memory_space=pltpu.VMEM)] * count


def comm_params(number):
    return pltpu.CompilerParams(
        collective_id=number, has_side_effects=True, vmem_limit_bytes=48 * 1024 * 1024
    )


def run_forward_exchange(number, normed, left, right, stream, gain):
    row_count, width = stream.shape
    return pl.pallas_call(
        functools.partial(forward_exchange, normed),
        out_shape=(
            jax.ShapeDtypeStruct((8, row_count, width), jnp.bfloat16),
            jax.ShapeDtypeStruct((row_count, width), jnp.float32),
        ),
        in_specs=vmem_specs(4),
        out_specs=tuple(vmem_specs(2)),
        scratch_shapes=scatter_scratch(row_count, width),
        compiler_params=comm_params(number),
        name="fwd_exchange_%d" % number,
    )(left, right, stream, gain)


def run_backward_exchange(number, spread, left, right, grad, stream, gain):
    row_count, width = stream.shape
    own = (
        jax.ShapeDtypeStruct((row_count, width), jnp.float32 if spread else jnp.bfloat16),
        jax.ShapeDtypeStruct((1, width), jnp.float32),
    )
    full = (jax.ShapeDtypeStruct((8, row_count, width), jnp.bfloat16),) if spread else ()
    return pl.pallas_call(
        functools.partial(backward_exchange, spread),
        out_shape=full + own,
        in_specs=vmem_specs(5),
        out_specs=tuple(vmem_specs(len(full + own))),
        scratch_shapes=scatter_scratch(row_count, width),
        compiler_params=comm_params(number),
        name="bwd_exchange_%d" % number,
    )(left, right, grad, stream, gain)


def opening(tokens, cotangent, gains, full_tokens, full_cotangent, full_gains,
            send_sem, recv_sem, send_two, recv_two, gain_send, gain_recv):
    place, mate, across, along = plane_neighbours()
    plane = lax.axis_index("shard")
    planes = lax.axis_size("shard")
    row_count = tokens.shape[0]
    others = [(plane + step) % planes for step in range(1, planes)]
    full_tokens[place] = tokens[...]
    full_cotangent[place] = cotangent[...]
    full_gains[plane] = gains[...]
    greet([{"rep": mate}, {"rep": across}, {"rep": along}] + [{"shard": other} for other in others])
    sent = [gather_send(full_tokens, (send_sem, recv_sem), 0, piece, row_count) for piece in range(PIECES)]
    gain_copies = []
    for step in range(1, planes):
        copy = pltpu.make_async_remote_copy(
            src_ref=full_gains.at[plane],
            dst_ref=full_gains.at[plane],
            send_sem=gain_send.at[step],
            recv_sem=gain_recv.at[step],
            device_id={"shard": others[step - 1]},
            device_id_type=MESH,
        )
        copy.start()
        gain_copies.append(copy)
    gather_finish(full_tokens, (send_sem, recv_sem), 0, row_count, sent)
    sent = [gather_send(full_cotangent, (send_two, recv_two), 0, piece, row_count) for piece in range(PIECES)]
    gather_finish(full_cotangent, (send_two, recv_two), 0, row_count, sent)
    for copy in gain_copies:
        copy.wait_recv()
        copy.wait_send()


def run_opening(number, tokens, cotangent, gains):
    row_count, width = tokens.shape
    planes = lax.axis_size("shard")
    full = jax.ShapeDtypeStruct((8, row_count, width), jnp.bfloat16)
    return pl.pallas_call(
        opening,
        out_shape=(full, full, jax.ShapeDtypeStruct((planes,) + gains.shape, gains.dtype)),
        in_specs=vmem_specs(3),
        out_specs=tuple(vmem_specs(3)),
        scratch_shapes=[pltpu.SemaphoreType.DMA((8, PIECES))] * 4
        + [pltpu.SemaphoreType.DMA((planes,))] * 2,
        compiler_params=comm_params(number),
        name="opening",
    )(tokens, cotangent, gains)


def plane_scores(queries, keys_rot, mask):
    scores = jnp.einsum(
        "sqhd,std->shqt", queries, keys_rot, preferred_element_type=jnp.float32
    ) * HEAD ** (-0.5)
    return jnp.where(mask, scores, masked_score)


def plane_attention(normed, weights, mask, cosine, sine):
    blocks, row_count, width = normed.shape
    heads = HEADS // blocks
    split = heads * HEAD
    mixed_in = left_product(normed.reshape(-1, width), weights).reshape(blocks, row_count, -1)
    queries = mixed_in[..., :split].reshape(blocks, row_count, heads, HEAD)
    queries = rotate(queries, cosine, sine).astype(jnp.bfloat16)
    keys_rot = rotate(mixed_in[..., split:split + HEAD], cosine[:, 0], sine[:, 0]).astype(jnp.bfloat16)
    values = mixed_in[..., split + HEAD:].astype(jnp.bfloat16)
    scores = plane_scores(queries, keys_rot, mask)
    row_max = jnp.max(scores, axis=-1, keepdims=True)
    shifted = jnp.exp(scores - row_max)
    row_total = jnp.sum(shifted, axis=-1, keepdims=True)
    attention = shifted / row_total
    log_total = row_max + jnp.log(row_total)
    mixed = jnp.einsum(
        "shqt,std->sqhd", attention.astype(jnp.bfloat16), values, preferred_element_type=jnp.float32
    )
    mixed = mixed.reshape(blocks, row_count, split).astype(jnp.bfloat16)
    return (mixed, (queries, keys_rot, values, log_total, mixed))


def plane_attention_back(mixed_grad, kept, mask, cosine, sine):
    queries, keys_rot, values, log_total, _ = kept
    blocks, row_count, heads, _ = queries.shape
    mixed_grad = mixed_grad.reshape(queries.shape)
    scores = plane_scores(queries, keys_rot, mask)
    attention = jnp.exp(scores - log_total)
    attention_grad = jnp.einsum("sqhd,std->shqt", mixed_grad, values, preferred_element_type=jnp.float32)
    value_grad = jnp.einsum(
        "shqt,sqhd->std", attention.astype(jnp.bfloat16), mixed_grad, preferred_element_type=jnp.float32
    ).astype(jnp.bfloat16)
    row_dot = jnp.sum(attention * attention_grad, axis=-1, keepdims=True)
    score_grad = (attention * (attention_grad - row_dot)).astype(jnp.bfloat16)
    query_grad = jnp.einsum(
        "shqt,std->sqhd", score_grad, keys_rot, preferred_element_type=jnp.float32
    ) * HEAD ** (-0.5)
    key_grad = jnp.einsum(
        "shqt,sqhd->std", score_grad, queries, preferred_element_type=jnp.float32
    ) * HEAD ** (-0.5)
    query_grad = unrotate(query_grad, cosine, sine).astype(jnp.bfloat16)
    key_grad = unrotate(key_grad, cosine[:, 0], sine[:, 0]).astype(jnp.bfloat16)
    return jnp.concatenate([query_grad.reshape(blocks, row_count, -1), key_grad, value_grad], axis=-1)


def plane_shards(
    tokens,
    cotangent,
    lengths,
    deal_order,
    attention_gain,
    query_weight,
    key_weight,
    value_weight,
    output_weight,
    feedforward_gain,
    gate_weight,
    up_weight,
    down_weight,
):
    place, plane = lax.axis_index("rep"), lax.axis_index("shard")
    places, planes = lax.axis_size("rep"), lax.axis_size("shard")
    row_count, width = tokens.shape[1:]
    share = width // planes
    heads = HEADS // places
    split = heads * HEAD
    hidden = gate_weight.shape[2]
    unit = hidden // places // planes
    head_plane = places // planes

    def head_columns(weight, layer, size):
        return lax.dynamic_slice_in_dim(weight[layer], place * size, size, 1)

    def unit_columns(weight, layer):
        parted = weight[layer].reshape(share, planes, places, unit)
        return lax.dynamic_index_in_dim(parted, place, 2, keepdims=False).reshape(share, planes * unit)

    def over_planes(piece):
        return lax.all_gather(piece, "shard", axis=0, tiled=True)

    def head_rows(layer):
        rows = lax.dynamic_slice_in_dim(
            output_weight[layer], (place % head_plane) * split, split, 0
        )
        arrived = jnp.where(plane == place // head_plane, rows, jnp.zeros_like(rows))
        for step in range(1, planes):
            pairs = [
                (spot * planes + spot // head_plane, spot * planes + (spot // head_plane + step) % planes)
                for spot in range(places)
            ]
            arrived = arrived + lax.ppermute(rows, ("rep", "shard"), pairs)
        return arrived

    projections, outputs, openers, downs = [], [], [], []
    for layer in range(LAYERS):
        projections.append(over_planes(jnp.concatenate(
            [head_columns(query_weight, layer, split), head_columns(key_weight, layer, HEAD),
             head_columns(value_weight, layer, HEAD)], axis=1)))
        outputs.append(head_rows(layer))
        openers.append(over_planes(jnp.concatenate(
            [unit_columns(gate_weight, layer), unit_columns(up_weight, layer)], axis=1)))
        downs.append(over_planes(lax.dynamic_slice_in_dim(down_weight[layer], place * unit, unit, 0)))

    gains = jnp.concatenate([attention_gain, feedforward_gain] * 2, axis=0).astype(jnp.float32)
    full_tokens, full_cotangent, full_gains = run_opening(0, tokens[0], cotangent[0], gains)
    full_gains = full_gains.transpose(1, 0, 2).reshape(-1, width)
    attend_gain = [full_gains[layer][None] for layer in range(LAYERS)]
    forward_gain = [full_gains[LAYERS + layer][None] for layer in range(LAYERS)]

    position = jnp.arange(row_count)
    spots = jnp.arange(places)
    plane_lengths = lengths[spots * planes + plane]
    valid = position[None, :] < plane_lengths[:, None]
    mask = (position[None, :] <= position[:, None])[None] & valid[:, None, :]
    mask = mask[:, None]
    cosine, sine = rope_tables(row_count)
    wanted = deal_order[spots * planes + plane] // planes
    inverse = jnp.sum(jnp.where(wanted[None, :] == spots[:, None], spots[None, :], 0), axis=1)
    branch_full = jnp.where(valid[:, :, None], full_cotangent[inverse], jnp.zeros((), jnp.bfloat16))
    own_valid = lax.dynamic_index_in_dim(valid, place, 0, keepdims=False)[:, None]
    grad = lax.dynamic_index_in_dim(branch_full, place, 0, keepdims=False).astype(jnp.float32)

    stream = tokens[0].astype(jnp.float32)
    wide = full_tokens.astype(jnp.float32)
    normed = (wide * norm_scale(wide) * attend_gain[0]).astype(jnp.bfloat16)
    kept = []
    ended = None
    for layer in range(LAYERS):
        mixed, attended = plane_attention(normed, projections[layer], mask, cosine, sine)
        normed_two, middle = run_forward_exchange(1, True, mixed, outputs[layer], stream, forward_gain[layer])
        both = left_product(normed_two.reshape(-1, width), openers[layer])
        gate_lin, up_lin = jnp.split(both.reshape(places, row_count, -1), 2, axis=-1)
        active = (gate_lin * jax.nn.sigmoid(gate_lin) * up_lin).astype(jnp.bfloat16)
        kept.append((stream, normed, attended, middle, normed_two, gate_lin, up_lin, active))
        if layer + 1 < LAYERS:
            normed, stream = run_forward_exchange(2, True, active, downs[layer], middle, attend_gain[layer + 1])
        else:
            ended, _ = run_forward_exchange(3, False, active, downs[layer], middle, attend_gain[layer])
    chosen = lax.dynamic_index_in_dim(wanted, place, 0, keepdims=False)
    chosen_valid = lax.dynamic_index_in_dim(valid, chosen, 0, keepdims=False)[:, None]
    layer_output = jnp.where(
        chosen_valid, lax.dynamic_index_in_dim(ended, chosen, 0, keepdims=False), jnp.zeros((), jnp.bfloat16)
    )[None]

    def summed(partial):
        return lax.psum_scatter(partial.astype(jnp.bfloat16), "shard", scatter_dimension=0, tiled=True)

    def over_places(piece):
        return lax.all_gather(piece, "rep", axis=0, tiled=False)

    def back_columns(gathered, parts):
        return gathered.reshape(places, share, parts, -1).transpose(1, 2, 0, 3).reshape(share, -1).astype(jnp.float32)

    layer_grads = [None] * LAYERS
    gain_parts = [None] * (2 * LAYERS)
    for layer in reversed(range(LAYERS)):
        stream, normed, attended, middle, normed_two, gate_lin, up_lin, active = kept[layer]
        flat = branch_full.reshape(-1, width)
        active_grad = right_transposed(flat, downs[layer]).reshape(active.shape)
        down_share = summed(row_sum_product(active.reshape(-1, active.shape[-1]), flat))
        sigma = jax.nn.sigmoid(gate_lin)
        gate_grad = (active_grad * up_lin * sigma * (1.0 + gate_lin * (1.0 - sigma))).astype(jnp.bfloat16)
        up_grad = (active_grad * gate_lin * sigma).astype(jnp.bfloat16)
        both_grad = jnp.concatenate([gate_grad, up_grad], axis=-1)
        opener_share = summed(row_sum_product(normed_two.reshape(-1, width), both_grad.reshape(places * row_count, -1)))
        branch_full, grad, gain_parts[LAYERS + layer] = run_backward_exchange(
            4, True, both_grad, openers[layer], grad, middle, forward_gain[layer])
        flat = branch_full.reshape(-1, width)
        mixed_grad = right_transposed(flat, outputs[layer]).astype(jnp.bfloat16)
        mixed = attended[-1]
        output_share = lax.psum(row_sum_product(mixed.reshape(-1, split), flat).astype(jnp.bfloat16), "shard")
        joint_grad = plane_attention_back(mixed_grad, attended, mask, cosine, sine)
        projection_share = summed(row_sum_product(normed.reshape(-1, width), joint_grad.reshape(places * row_count, -1)))
        if layer > 0:
            branch_full, grad, gain_parts[layer] = run_backward_exchange(
                5, True, joint_grad, projections[layer], grad, stream, attend_gain[layer])
        else:
            input_grad, gain_parts[layer] = run_backward_exchange(
                6, False, joint_grad, projections[layer], grad, stream, attend_gain[layer])
        down_grad = over_places(down_share).reshape(places * unit, width).astype(jnp.float32)
        opener_full = over_places(opener_share)
        gate_weight_grad = back_columns(opener_full[..., :planes * unit], planes)
        up_weight_grad = back_columns(opener_full[..., planes * unit:], planes)
        output_full = over_places(output_share).reshape(places * split, width)
        output_grad = lax.dynamic_slice_in_dim(output_full, plane * share, share, 0).astype(jnp.float32)
        projection_full = over_places(projection_share)
        query_grad = back_columns(projection_full[..., :split], 1)
        key_grad = back_columns(projection_full[..., split:split + HEAD], 1)
        value_grad = back_columns(projection_full[..., split + HEAD:], 1)
        layer_grads[layer] = (query_grad, key_grad, value_grad, output_grad, gate_weight_grad, up_weight_grad, down_grad)

    gain_sum = lax.psum(jnp.concatenate(gain_parts, axis=0), ("rep", "shard"))
    gain_sum = lax.dynamic_slice_in_dim(gain_sum, plane * share, share, 1)
    stacked = [jnp.stack([layer_grads[layer][member] for layer in range(LAYERS)]) for member in range(7)]
    return (
        layer_output,
        input_grad[None],
        gain_sum[:LAYERS],
        stacked[0],
        stacked[1],
        stacked[2],
        stacked[3],
        gain_sum[LAYERS:],
        stacked[4],
        stacked[5],
        stacked[6],
    )


def solution(mesh):
    placed = (
        P(("rep", "shard"), None, None),
        P(("rep", "shard"), None, None),
        P(),
        P(),
        P(None, "shard"),
        P(None, "shard", None),
        P(None, "shard", None),
        P(None, "shard", None),
        P(None, "shard", None),
        P(None, "shard"),
        P(None, "shard", None),
        P(None, "shard", None),
        P(None, "shard", None),
    )
    split_heads = mesh.shape["rep"] == KV_HEADS and mesh.shape["rep"] % mesh.shape["shard"] == 0
    return jax.shard_map(
        plane_shards if split_heads else whole_weight_shards,
        mesh=mesh,
        in_specs=placed,
        out_specs=(
            P(("rep", "shard"), None, None),
            P(("rep", "shard"), None, None),
            P(None, "shard"),
            P(None, "shard", None),
            P(None, "shard", None),
            P(None, "shard", None),
            P(None, "shard", None),
            P(None, "shard"),
            P(None, "shard", None),
            P(None, "shard", None),
            P(None, "shard", None),
        ),
        check_vma=False,
    )
```
